16 devices in a mesh: rep: 4 (over y, z, core), dp: 4 (over x).
Axes of the slice: x: 4, y: 2, z: 1, core: 2. Of those that a mesh axis runs over, the one named last changes fastest.
The devices are a block of a 4x4x8 slice.
Arguments:
- x: bfloat16 [16, 4096, 512], P(('rep', 'dp')), parts along dimension 0
- dy: bfloat16 [16, 4096, 512], P(('rep', 'dp')), parts along dimension 0
- w_gate: bfloat16 [2, 512, 3072], replicated
- w_up: bfloat16 [2, 512, 3072], replicated
- w_down: bfloat16 [2, 3072, 512], replicated
- m_w_gate: float32 [2, 512, 3072], P(None, 'dp')
- m_w_up: float32 [2, 512, 3072], P(None, 'dp')
- m_w_down: float32 [2, 3072, 512], P(None, 'dp')
- v_w_gate: float32 [2, 512, 3072], P(None, 'dp')
- v_w_up: float32 [2, 512, 3072], P(None, 'dp')
- v_w_down: float32 [2, 3072, 512], P(None, 'dp')
Outputs:
- output 1: bfloat16 [8, 512, 3072], P('rep'), parts along dimension 0
- output 2: bfloat16 [8, 512, 3072], P('rep'), parts along dimension 0
- output 3: bfloat16 [8, 3072, 512], P('rep'), parts along dimension 0
- output 4: float32 [8, 512, 3072], P('rep', 'dp'), parts along dimension 0
- output 5: float32 [8, 512, 3072], P('rep', 'dp'), parts along dimension 0
- output 6: float32 [8, 3072, 512], P('rep', 'dp'), parts along dimension 0
- output 7: float32 [8, 512, 3072], P('rep', 'dp'), parts along dimension 0
- output 8: float32 [8, 512, 3072], P('rep', 'dp'), parts along dimension 0
- output 9: float32 [8, 3072, 512], P('rep', 'dp'), parts along dimension 0
There are 4 independent parts. The reference program is written for one: setup_inputs(seed, part) draws one part's arguments, and reference() takes and returns one part's arrays. A program takes and returns all parts, laid end to end along the dimension named above; an argument that names none is the same for every part.
All inputs are finite; a program needn't handle non-finite values.
Results may differ from the reference program's by a relative error of at most 0.022.
Values are sent between devices in bfloat16 or wider.
A program may use at most 768 MiB of HBM per device.

```python
import jax
import jax.numpy as jnp
from jax import lax

SEQUENCES = 4
TOKENS = 4096
D = 512
FF = 3072
LAYERS = 2
NAMES = ("w_gate", "w_up", "w_down")
SHAPES = {"w_gate": (LAYERS, D, FF), "w_up": (LAYERS, D, FF), "w_down": (LAYERS, FF, D)}


def bump(key, n, height):
    away = (jnp.arange(n, dtype=jnp.int32) - jax.random.randint(key, (), 0, n, jnp.int32)) % n
    return jnp.where(away < n // 8, height, 1.0)


def together(key, own, strength):
    shared = jax.random.normal(key, own.shape[1:], jnp.float32)
    return (own + strength * shared) * lax.rsqrt(1 + strength * strength)


def setup_inputs(seed: int = 0, part: int = 0) -> dict:
    kx, kdy, ka, kb, kz, kf, kh, kl, *keys = jax.random.split(jax.random.key(seed), 8 + 3 * len(NAMES))
    kx, kdy, ka, kb = (jax.random.fold_in(k, part) for k in (kx, kdy, ka, kb))
    kw, km, kv = (keys[i::3] for i in range(3))
    shape = (SEQUENCES, TOKENS, D)
    much_x, much_dy = jax.random.uniform(kz, (2,), jnp.float32, 0.0, 1.0)
    loud = 2.0 ** jax.random.uniform(jax.random.fold_in(kz, 1), (), jnp.float32, -1.0, 2.0)
    layers = 2.0 ** jax.random.uniform(kl, (LAYERS, 1, 1), jnp.float32, -1.0, 1.0)
    x = together(ka, jax.random.normal(kx, shape, jnp.float32), much_x) * bump(kf, D, 4.0)
    dy = together(kb, jax.random.normal(kdy, shape, jnp.float32), much_dy)
    drawn = {"x": x.astype(jnp.bfloat16), "dy": (loud * dy * (SEQUENCES * TOKENS) ** -0.5).astype(jnp.bfloat16)}
    for key, name in zip(kw, NAMES, strict=True):
        w = jax.random.normal(key, SHAPES[name], jnp.float32) * SHAPES[name][1] ** -0.5
        drawn[name] = (w * {"w_gate": 1.0, "w_up": bump(kh, FF, 4.0), "w_down": layers}[name]).astype(jnp.bfloat16)
    for key, name in zip(km, NAMES, strict=True):
        drawn[f"m_{name}"] = 0.1 * jax.random.normal(key, SHAPES[name], jnp.float32)
    for key, name in zip(kv, NAMES, strict=True):
        drawn[f"v_{name}"] = jax.random.uniform(key, SHAPES[name], jnp.float32, 0.005, 0.015)
    return drawn


def matmul(a, w):
    return jnp.dot(a, w, preferred_element_type=jnp.float32).astype(jnp.bfloat16)


def normed(h):
    wide = h.astype(jnp.float32)
    scale = lax.rsqrt(jnp.mean(wide**2, -1, keepdims=True) + 1e-6)
    return (wide * scale).astype(jnp.bfloat16)


def layer(h, w):
    a = normed(h)
    gate = jnp.dot(a, w["w_gate"], preferred_element_type=jnp.float32)
    up = jnp.dot(a, w["w_up"], preferred_element_type=jnp.float32)
    return h + matmul((jax.nn.silu(gate) * up).astype(jnp.bfloat16), w["w_down"])


def adamw(w, m, v, g):
    m = 0.9 * m + 0.1 * g
    v = 0.95 * v + 0.05 * g * g
    step = m * lax.rsqrt(v + 1e-8) + 0.1 * w
    return (w - 0.02 * step).astype(jnp.bfloat16), m, v


def stack(weights, h):
    return lax.scan(lambda h, w: (layer(h, w), None), h, weights)[0]


def reference(x, dy, w_gate, w_up, w_down, m_w_gate, m_w_up, m_w_down, v_w_gate, v_w_up, v_w_down):
    weights = dict(zip(NAMES, (w_gate, w_up, w_down), strict=True))

    def take(so_far, sequence):
        h, by_y = sequence
        _, back = jax.vjp(lambda w: stack(w, h), weights)
        return jax.tree.map(lambda total, term: total + term.astype(jnp.float32), so_far, back(by_y)[0]), None

    none_yet = {name: jnp.zeros(w.shape, jnp.float32) for name, w in weights.items()}
    by_weights, _ = lax.scan(take, none_yet, (x, dy))
    gradients = [by_weights[name].astype(jnp.bfloat16).astype(jnp.float32) for name in NAMES]
    new = [
        adamw(w.astype(jnp.float32), m, v, g)
        for w, m, v, g in zip((w_gate, w_up, w_down), (m_w_gate, m_w_up, m_w_down), (v_w_gate, v_w_up, v_w_down), gradients, strict=True)
    ]
    return tuple(one[which] for which in range(3) for one in new)
```

```python
import functools

import jax
import jax.numpy as jnp
from jax import lax
from jax.experimental import pallas as pl
from jax.experimental.pallas import tpu as pltpu
from jax.sharding import PartitionSpec as P

F32, BF16 = jnp.float32, jnp.bfloat16
MESH = pl.DeviceIdType.MESH
PIECE = 128
TF = 512
TB = 1024
SUB = 512
VMEM = 60 * 1024 * 1024


def dot(a, b):
    return jnp.dot(a, b, preferred_element_type=F32)


def dot_nt(a, b):
    return lax.dot_general(a, b, (((1,), (1,)), ((), ())), preferred_element_type=F32)


def normed(h):
    wide = h.astype(F32)
    scale = lax.rsqrt(jnp.mean(wide * wide, -1, keepdims=True) + 1e-6)
    return (wide * scale).astype(BF16)


def fwd_kernel(x_ref, dy_ref, wg_ref, wu_ref, wd_ref, h_ref, a_ref, at_ref, dyt_ref):
    x = x_ref[0]
    a = normed(x)
    a_ref[0] = a
    at_ref[0] = a.T
    dyt_ref[...] = dy_ref[0].T
    acc = None
    for c in range(wg_ref.shape[2] // 512):
        cols = pl.ds(c * 512, 512)
        gate = dot(a, wg_ref[0, :, cols])
        up = dot(a, wu_ref[0, :, cols])
        p = (gate * lax.logistic(gate) * up).astype(BF16)
        part = dot(p, wd_ref[0, cols, :])
        acc = part if acc is None else acc + part
    h = x + acc.astype(BF16)
    h_ref[...] = h
    a2 = normed(h)
    a_ref[1] = a2
    at_ref[1] = a2.T


def forward(x, dy, wg, wu, wd):
    _, tokens, d = x.shape
    ff = wg.shape[2]
    tok = pl.BlockSpec((TF, d), lambda t: (t, 0))
    tokt = pl.BlockSpec((d, TF), lambda t: (0, t))
    tok3 = pl.BlockSpec((1, TF, d), lambda t: (0, t, 0))
    both = pl.BlockSpec((2, TF, d), lambda t: (0, t, 0))
    botht = pl.BlockSpec((2, d, TF), lambda t: (0, 0, t))
    wcol = pl.BlockSpec((1, d, ff), lambda t: (0, 0, 0))
    wrow = pl.BlockSpec((1, ff, d), lambda t: (0, 0, 0))
    shape = lambda *s: jax.ShapeDtypeStruct(s, BF16)
    return pl.pallas_call(
        fwd_kernel,
        grid=(tokens // TF,),
        in_specs=[tok3, tok3, wcol, wcol, wrow],
        out_specs=[tok, both, botht, tokt],
        out_shape=[shape(tokens, d), shape(2, tokens, d), shape(2, d, tokens), shape(d, tokens)],
        compiler_params=pltpu.CompilerParams(vmem_limit_bytes=VMEM, dimension_semantics=("arbitrary",)),
        cost_estimate=pl.CostEstimate(flops=6 * tokens * d * ff, bytes_accessed=2 * (8 * tokens * d + 3 * d * ff), transcendentals=tokens * ff),
        name="forward",
    )(x, dy, wg, wu, wd)


def step_of_adamw(w, m, v, g):
    m = 0.9 * m + 0.1 * g
    v = 0.95 * v + 0.05 * g * g
    w = w.astype(F32)
    return (w - 0.02 * (m * lax.rsqrt(v + 1e-8) + 0.1 * w)).astype(BF16)


def bwd_kernel(n, per_layer, *refs):
    refs = list(refs)
    take = lambda k: [refs.pop(0) for _ in range(k)]
    a_ref, at_ref, h_ref = take(3)
    wg_refs, wu_refs, wd_refs = take(n), take(n), take(n)
    dy_hbm, dyt_hbm, wg_hbm, wu_hbm, wd_hbm, mg_hbm, mu_hbm, md_hbm, vg_hbm, vu_hbm, vd_hbm = take(11)
    wag, gs = take(2)
    d_s, dt_s, da_s, wg_s, wu_s, wd_s, accg, accu, accd = take(9)
    grads, far_a, far_b, near_a, near_b, new_s, gst, w_st, m_st, v_st = take(10)
    init_sem, send_sem, recv_sem, st_sem, gs_sem, own_sem = take(6)

    u, t = pl.program_id(0), pl.program_id(1)
    nt = pl.num_programs(1)
    units = 2 * per_layer
    dm, f = accg.shape
    half = PIECE // 2
    share = per_layer * PIECE
    me = lax.axis_index("dp")
    right, left, across = lax.rem(me + 1, n), lax.rem(me + n - 1, n), lax.rem(me + 2, n)

    def remote(kind, par, src, dst, to):
        return pltpu.make_async_remote_copy(
            src_ref=src, dst_ref=dst, send_sem=send_sem.at[kind, par], recv_sem=recv_sem.at[kind, par], device_id={"dp": to}, device_id_type=MESH
        )

    low, high = pl.ds(0, half), pl.ds(half, half)

    def far(par):
        return (
            remote(0, par, grads.at[par, across, :, low, :], far_a.at[par], right),
            remote(1, par, grads.at[par, across, :, high, :], far_b.at[par], left),
        )

    def near(par):
        return (
            remote(2, par, grads.at[par, right], near_a.at[par], right),
            remote(3, par, grads.at[par, left], near_b.at[par], left),
        )

    def out_near(unit, par):
        return (
            remote(4, par, new_s.at[par], wag.at[unit, me], right),
            remote(5, par, new_s.at[par], wag.at[unit, me], left),
        )

    def out_far(unit, par):
        return (
            remote(6, par, wag.at[unit, left, :, low, :], wag.at[unit, left, :, low, :], right),
            remote(7, par, wag.at[unit, right, :, high, :], wag.at[unit, right, :, high, :], left),
        )

    def own_copy(unit, par):
        return pltpu.make_async_copy(new_s.at[par], wag.at[unit, me], own_sem.at[par])

    def gs_copy(unit, par):
        return pltpu.make_async_copy(gst.at[par], gs.at[unit], gs_sem.at[par])

    def stage(unit):
        layer = jnp.where(unit < per_layer, 1, 0)
        at = lax.rem(unit, per_layer) * PIECE
        rows = pl.ds(pl.multiple_of(me * (dm // n), dm // n), dm // n)
        copies = []
        for k, (w, m, v) in enumerate(((wg_hbm, mg_hbm, vg_hbm), (wu_hbm, mu_hbm, vu_hbm))):
            for d in range(n):
                cols = pl.ds(pl.multiple_of(d * share + at, PIECE), PIECE)
                to = pl.ds(d * PIECE, PIECE)
                copies += [(w.at[layer, rows, cols], w_st.at[k, :, to]), (m.at[layer, :, cols], m_st.at[k, :, to]), (v.at[layer, :, cols], v_st.at[k, :, to])]
        own = pl.ds(pl.multiple_of(at, PIECE), PIECE)
        copies += [
            (wd_hbm.at[layer, pl.ds(pl.multiple_of(me * share + at, PIECE), PIECE), :], w_st.at[2]),
            (md_hbm.at[layer, own, :], m_st.at[2]),
            (vd_hbm.at[layer, own, :], v_st.at[2]),
        ]
        return [pltpu.make_async_copy(src, dst, st_sem.at[i]) for i, (src, dst) in enumerate(copies)]

    def slot(i):
        unit, older = u - 1, u - 2
        par, opar = lax.rem(unit + 2, 2), lax.rem(older + 2, 2)
        summing = (unit >= 0) & (unit < units)
        sharing = (older >= 0) & (older < units)
        if i != 0:
            return

        @pl.when((t == 0) & summing)
        def _():
            for copy in far(par):
                copy.start()

        @pl.when((t == 1) & summing)
        def _():
            for copy in far(par):
                copy.wait()
            for to, part, got in ((right, low, far_a), (left, high, far_b)):
                total = grads[par, to, :, part, :].astype(F32) + got[par].astype(F32)
                grads[par, to, :, part, :] = total.astype(BF16)
            for copy in near(par):
                copy.start()
            for copy in stage(unit):
                copy.start()

        @pl.when((t == 1) & sharing)
        def _():
            for copy in out_near(older, opar):
                copy.wait()
            own_copy(older, opar).wait()
            for copy in out_far(older, opar):
                copy.start()

        @pl.when((t == 3) & summing)
        def _():
            for copy in near(par):
                copy.wait()
            for copy in stage(unit):
                copy.wait()

            @pl.when(unit >= 2)
            def _():
                gs_copy(unit - 2, par).wait()

            for k in range(3):
                total = grads[par, me, k].astype(F32) + near_a[par, k].astype(F32) + near_b[par, k].astype(F32)
                total = total.astype(BF16)
                gst[par, k] = total
                new_s[par, k] = step_of_adamw(w_st[k], m_st[k], v_st[k], total.astype(F32))
            for copy in out_near(unit, par):
                copy.start()
            own_copy(unit, par).start()
            gs_copy(unit, par).start()

        @pl.when((t == 3) & sharing)
        def _():
            for copy in out_far(older, opar):
                copy.wait()

        @pl.when((t == 3) & (u == units + 1))
        def _():
            gs_copy(units - 2, 0).wait()
            gs_copy(units - 1, 1).wait()

    def init(k):
        rows = pl.ds(pl.multiple_of(k * TB, TB), TB)
        return (
            pltpu.make_async_copy(dy_hbm.at[0, rows, :], d_s.at[rows, :], init_sem.at[0, k]),
            pltpu.make_async_copy(dyt_hbm.at[:, rows], dt_s.at[:, rows], init_sem.at[1, k]),
        )

    @pl.when((u == 0) & (t == 0))
    def _():
        for k in range(d_s.shape[0] // TB):
            for copy in init(k):
                copy.start()
        barrier = pltpu.get_barrier_semaphore()
        for to in (left, right):
            pl.semaphore_signal(barrier, inc=1, device_id={"dp": to}, device_id_type=MESH)
        pl.semaphore_wait(barrier, 2)

    @pl.when(u == 0)
    def _():
        for copy in init(t):
            copy.wait()

    @pl.when((u < units) & (t == 0))
    def _():
        accg[...] = jnp.zeros_like(accg)
        accu[...] = jnp.zeros_like(accu)
        accd[...] = jnp.zeros_like(accd)
        for k in range(n):
            to = pl.ds(k * PIECE, PIECE)
            wg_s[:, to] = wg_refs[k][0]
            wu_s[:, to] = wu_refs[k][0]
            wd_s[to, :] = wd_refs[k][0]

    here = pl.ds(pl.multiple_of(t * TB, TB), TB)

    @pl.when(u == 0)
    def _():
        da_s[here, :] = jnp.zeros((TB, dm), F32)

    def compute(i, with_da):
        rows = pl.ds(i * SUB, SUB)
        sub = pl.ds(pl.multiple_of(t * TB + i * SUB, SUB), SUB)
        wg, wu, wd = wg_s[...], wu_s[...], wd_s[...]
        a, d = a_ref[0, rows, :], d_s[sub, :]
        gate = dot(a, wg)
        up = dot(a, wu)
        dp = dot_nt(d, wd).astype(BF16).astype(F32)
        s = lax.logistic(gate)
        silu = gate * s
        p = (silu * up).astype(BF16)
        dup = (dp * silu).astype(BF16)
        dgate = (dp * up * (s + silu * (1.0 - s))).astype(BF16)
        at = at_ref[0, :, rows]
        accg[...] += dot(at, dgate)
        accu[...] += dot(at, dup)
        accd[...] += dot(dt_s[:, sub], p)
        if with_da:
            da_s[sub, :] += dot_nt(dgate, wg) + dot_nt(dup, wu)

    slot(0)

    @pl.when(u < per_layer)
    def _():
        for i in range(TB // SUB):
            compute(i, True)

    @pl.when((u >= per_layer) & (u < units))
    def _():
        for i in range(TB // SUB):
            compute(i, False)

    @pl.when((u < units) & (t == nt - 1))
    def _():
        par = lax.rem(u, 2)
        for k in range(n):
            part = pl.ds(k * PIECE, PIECE)
            grads[par, k, 0] = accg[part, :].astype(BF16)
            grads[par, k, 1] = accu[part, :].astype(BF16)
            grads[par, k, 2] = accd[:, part].astype(BF16).T

    @pl.when(u == per_layer - 1)
    def _():
        da = da_s[here, :].astype(BF16).astype(F32)
        wide = h_ref[...].astype(F32)
        scale = lax.rsqrt(jnp.mean(wide * wide, -1, keepdims=True) + 1e-6)
        along = jnp.mean(da * wide, -1, keepdims=True)
        dn = (da * scale - wide * (along * (scale * scale * scale))).astype(BF16)
        dh = d_s[here, :] + dn
        d_s[here, :] = dh
        dt_s[:, here] = dh.T


def backward(n, a, at, h, dy, dyt, wg, wu, wd, moments):
    _, tokens, dm = a.shape
    layers, _, ff = wg.shape
    nt = tokens // TB
    f = n * PIECE
    per_layer = ff // f
    units = layers * per_layer
    now = lambda u: jnp.minimum(u, units - 1)
    layer = lambda u: jnp.where(u < per_layer, 1, 0)
    piece = lambda k: lambda u, t: (layer(u), 0, k * per_layer + lax.rem(now(u), per_layer))
    piece_t = lambda k: lambda u, t: (layer(u), k * per_layer + lax.rem(now(u), per_layer), 0)
    step = lambda u, t: jnp.where(u < units, t, nt - 1)
    hbm = pl.BlockSpec(memory_space=pl.ANY)
    in_specs = [
        pl.BlockSpec((1, TB, dm), lambda u, t: (layer(u), step(u, t), 0)),
        pl.BlockSpec((1, dm, TB), lambda u, t: (layer(u), 0, step(u, t))),
        pl.BlockSpec((TB, dm), lambda u, t: (jnp.where(u == per_layer - 1, t, jnp.where(u < per_layer, 0, nt - 1)), 0)),
        *[pl.BlockSpec((1, dm, PIECE), piece(k)) for k in range(n)] * 1,
        *[pl.BlockSpec((1, dm, PIECE), piece(k)) for k in range(n)],
        *[pl.BlockSpec((1, PIECE, dm), piece_t(k)) for k in range(n)],
        *[hbm] * 11,
    ]
    chunk = (3, PIECE, dm)
    part = (3, PIECE // 2, dm)
    dma = pltpu.SemaphoreType.DMA
    return pl.pallas_call(
        functools.partial(bwd_kernel, n, per_layer),
        grid=(units + 2, nt),
        in_specs=in_specs,
        out_specs=[hbm, hbm],
        out_shape=[jax.ShapeDtypeStruct((units, n, *chunk), BF16), jax.ShapeDtypeStruct((units, *chunk), BF16)],
        scratch_shapes=[
            pltpu.VMEM((tokens, dm), BF16),
            pltpu.VMEM((dm, tokens), BF16),
            pltpu.VMEM((tokens, dm), F32),
            pltpu.VMEM((dm, f), BF16),
            pltpu.VMEM((dm, f), BF16),
            pltpu.VMEM((f, dm), BF16),
            pltpu.VMEM((dm, f), F32),
            pltpu.VMEM((dm, f), F32),
            pltpu.VMEM((dm, f), F32),
            pltpu.VMEM((2, n, *chunk), BF16),
            pltpu.VMEM((2, *part), BF16),
            pltpu.VMEM((2, *part), BF16),
            pltpu.VMEM((2, *chunk), BF16),
            pltpu.VMEM((2, *chunk), BF16),
            pltpu.VMEM((2, *chunk), BF16),
            pltpu.VMEM((2, *chunk), BF16),
            pltpu.VMEM(chunk, BF16),
            pltpu.VMEM(chunk, F32),
            pltpu.VMEM(chunk, F32),
            dma((2, nt)),
            dma((8, 2)),
            dma((8, 2)),
            dma((6 * n + 3,)),
            dma((2,)),
            dma((2,)),
        ],
        compiler_params=pltpu.CompilerParams(
            vmem_limit_bytes=VMEM, dimension_semantics=("arbitrary", "arbitrary"), collective_id=0, has_side_effects=True
        ),
        cost_estimate=pl.CostEstimate(flops=14 * layers * tokens * dm * ff, bytes_accessed=12 * tokens * ff, transcendentals=layers * tokens * ff),
        name="backward",
    )(a, at, h, *[wg] * n, *[wu] * n, *[wd] * n, dy, dyt, wg, wu, wd, *moments)


def finish_kernel(n, per_layer, wag, gs, *refs):
    olds, outs = refs[:6], refs[6:]
    q = pl.program_id(1)
    share = per_layer * PIECE
    rows = outs[3].shape[1]
    lanes = outs[5].shape[2]
    mine = pl.ds(pl.multiple_of(q * rows, rows), rows)
    some = pl.ds(pl.multiple_of(q * lanes, lanes), lanes)

    def moments(k, where, g):
        g = g.astype(F32)
        outs[3 + k][where] = 0.9 * olds[k][where] + 0.1 * g
        outs[6 + k][where] = 0.95 * olds[3 + k][where] + 0.05 * g * g

    for j in range(per_layer):
        down = pl.ds(j * PIECE, PIECE)
        outs[2][0, down, :] = wag[j, 0, 2]
        moments(2, (0, down, slice(None)), gs[j, 2, :, some])
        for d in range(n):
            cols = pl.ds(d * share + j * PIECE, PIECE)
            for k in range(2):
                outs[k][0, :, cols] = wag[j, 0, k, :, d * PIECE : (d + 1) * PIECE]
                moments(k, (0, slice(None), cols), gs[j, k, mine, d * PIECE : (d + 1) * PIECE])


def finish(n, wag, gs, olds):
    units, _, _, _, dm = wag.shape
    layers, rows, ff = olds[0].shape
    per_layer = units // layers
    share = per_layer * PIECE
    small = [pl.BlockSpec((1, rows // n, ff), lambda l, q: (l, q, 0))] * 2 + [pl.BlockSpec((1, share, dm // n), lambda l, q: (l, 0, q))]
    whole = [pl.BlockSpec((1, rows, ff), lambda l, q: (l, q, 0))] * 2 + [pl.BlockSpec((1, share, dm), lambda l, q: (l, q, 0))]
    return pl.pallas_call(
        functools.partial(finish_kernel, n, per_layer),
        grid=(layers, n),
        in_specs=[
            pl.BlockSpec((per_layer, 1, 3, PIECE, dm), lambda l, q: (layers - 1 - l, q, 0, 0, 0)),
            pl.BlockSpec((per_layer, 3, PIECE, dm), lambda l, q: (layers - 1 - l, 0, 0, 0)),
            *small,
            *small,
        ],
        out_specs=[*whole, *small, *small],
        out_shape=[jax.ShapeDtypeStruct((layers, dm, ff), BF16)] * 2
        + [jax.ShapeDtypeStruct((layers, ff, dm), BF16)]
        + [jax.ShapeDtypeStruct(one.shape, F32) for one in olds],
        compiler_params=pltpu.CompilerParams(vmem_limit_bytes=VMEM, dimension_semantics=("arbitrary", "arbitrary")),
        name="finish",
    )(wag, gs, *olds)


def solution(mesh):
    n = mesh.shape["dp"]

    def step(x, dy, wg, wu, wd, *olds):
        h, a, at, dyt = forward(x, dy, wg, wu, wd)
        wag, gs = backward(n, a, at, h, dy, dyt, wg, wu, wd, olds)
        return tuple(finish(n, wag, gs, olds))

    whole = P(None, None, None)
    rows = P(None, "dp", None)
    seq = P(("rep", "dp"), None, None)
    return jax.shard_map(
        step,
        mesh=mesh,
        in_specs=(seq, seq, whole, whole, whole, *[rows] * 6),
        out_specs=(*[P("rep", None, None)] * 3, *[P("rep", "dp", None)] * 6),
        check_vma=False,
    )
```

```python
import functools

import jax
import jax.numpy as jnp
from jax import lax
from jax.experimental import pallas as pl
from jax.experimental.pallas import tpu as pltpu
from jax.sharding import PartitionSpec as P

F32, BF16 = jnp.float32, jnp.bfloat16
MESH = pl.DeviceIdType.MESH
PIECE = 128
TF = 512
TB = 1024
SUB = 512
VMEM = 60 * 1024 * 1024


def dot(a, b):
    return jnp.dot(a, b, preferred_element_type=F32)


def dot_nt(a, b):
    return lax.dot_general(a, b, (((1,), (1,)), ((), ())), preferred_element_type=F32)


def normed(h):
    wide = h.astype(F32)
    scale = lax.rsqrt(jnp.mean(wide * wide, -1, keepdims=True) + 1e-6)
    return (wide * scale).astype(BF16)


def fwd_kernel(x_ref, dy_ref, wg_ref, wu_ref, wd_ref, h_ref, a_ref, at_ref, dyt_ref):
    x = x_ref[0]
    a = normed(x)
    a_ref[0] = a
    at_ref[0] = a.T
    dyt_ref[...] = dy_ref[0].T
    acc = None
    for c in range(wg_ref.shape[2] // 512):
        cols = pl.ds(c * 512, 512)
        gate = dot(a, wg_ref[0, :, cols])
        up = dot(a, wu_ref[0, :, cols])
        p = (gate * lax.logistic(gate) * up).astype(BF16)
        part = dot(p, wd_ref[0, cols, :])
        acc = part if acc is None else acc + part
    h = x + acc.astype(BF16)
    h_ref[...] = h
    a2 = normed(h)
    a_ref[1] = a2
    at_ref[1] = a2.T


def forward(x, dy, wg, wu, wd):
    _, tokens, d = x.shape
    ff = wg.shape[2]
    tok = pl.BlockSpec((TF, d), lambda t: (t, 0))
    tokt = pl.BlockSpec((d, TF), lambda t: (0, t))
    tok3 = pl.BlockSpec((1, TF, d), lambda t: (0, t, 0))
    both = pl.BlockSpec((2, TF, d), lambda t: (0, t, 0))
    botht = pl.BlockSpec((2, d, TF), lambda t: (0, 0, t))
    wcol = pl.BlockSpec((1, d, ff), lambda t: (0, 0, 0))
    wrow = pl.BlockSpec((1, ff, d), lambda t: (0, 0, 0))
    shape = lambda *s: jax.ShapeDtypeStruct(s, BF16)
    return pl.pallas_call(
        fwd_kernel,
        grid=(tokens // TF,),
        in_specs=[tok3, tok3, wcol, wcol, wrow],
        out_specs=[tok, both, botht, tokt],
        out_shape=[shape(tokens, d), shape(2, tokens, d), shape(2, d, tokens), shape(d, tokens)],
        compiler_params=pltpu.CompilerParams(vmem_limit_bytes=VMEM, dimension_semantics=("arbitrary",)),
        cost_estimate=pl.CostEstimate(flops=6 * tokens * d * ff, bytes_accessed=2 * (8 * tokens * d + 3 * d * ff), transcendentals=tokens * ff),
        name="forward",
    )(x, dy, wg, wu, wd)


def step_of_adamw(w, m, v, g):
    m = 0.9 * m + 0.1 * g
    v = 0.95 * v + 0.05 * g * g
    w = w.astype(F32)
    return (w - 0.02 * (m * lax.rsqrt(v + 1e-8) + 0.1 * w)).astype(BF16)


def bwd_kernel(n, per_layer, *refs):
    refs = list(refs)
    take = lambda k: [refs.pop(0) for _ in range(k)]
    a_ref, at_ref, h_ref = take(3)
    wg_refs, wu_refs, wd_refs = take(n), take(n), take(n)
    dy_hbm, dyt_hbm, wg_hbm, wu_hbm, wd_hbm, mg_hbm, mu_hbm, md_hbm, vg_hbm, vu_hbm, vd_hbm = take(11)
    wag, gs = take(2)
    d_s, dt_s, da_s, wg_s, wu_s, wd_s, accg, accu, accd = take(9)
    grads, far_a, far_b, near_a, near_b, new_s, gst, w_st, m_st, v_st = take(10)
    init_sem, send_sem, recv_sem, st_sem, gs_sem, own_sem = take(6)

    u, t = pl.program_id(0), pl.program_id(1)
    nt = pl.num_programs(1)
    units = 2 * per_layer
    dm, f = accg.shape
    half = PIECE // 2
    share = per_layer * PIECE
    me = lax.axis_index("dp")
    right, left, across = lax.rem(me + 1, n), lax.rem(me + n - 1, n), lax.rem(me + 2, n)

    def remote(kind, par, src, dst, to):
        return pltpu.make_async_remote_copy(
            src_ref=src, dst_ref=dst, send_sem=send_sem.at[kind, par], recv_sem=recv_sem.at[kind, par], device_id={"dp": to}, device_id_type=MESH
        )

    low, high = pl.ds(0, half), pl.ds(half, half)

    def far(par):
        return (
            remote(0, par, grads.at[par, across, :, low, :], far_a.at[par], right),
            remote(1, par, grads.at[par, across, :, high, :], far_b.at[par], left),
        )

    def plain(par):
        return (
            remote(2, par, grads.at[par, right, :, high, :], near_a.at[par, :, high, :], right),
            remote(3, par, grads.at[par, left, :, low, :], near_b.at[par, :, low, :], left),
        )

    def joined(par):
        return (
            remote(4, par, grads.at[par, right, :, low, :], near_a.at[par, :, low, :], right),
            remote(5, par, grads.at[par, left, :, high, :], near_b.at[par, :, high, :], left),
        )

    def out_first(unit, par):
        return (
            remote(6, par, new_s.at[par, :, low, :], wag.at[unit, me, :, low, :], right),
            remote(7, par, new_s.at[par, :, high, :], wag.at[unit, me, :, high, :], left),
        )

    def out_second(unit, par):
        return (
            remote(8, par, new_s.at[par, :, high, :], wag.at[unit, me, :, high, :], right),
            remote(9, par, new_s.at[par, :, low, :], wag.at[unit, me, :, low, :], left),
        )

    def out_far(unit, par):
        return (
            remote(10, par, wag.at[unit, left, :, low, :], wag.at[unit, left, :, low, :], right),
            remote(11, par, wag.at[unit, right, :, high, :], wag.at[unit, right, :, high, :], left),
        )

    def own_copy(unit, par):
        return pltpu.make_async_copy(new_s.at[par], wag.at[unit, me], own_sem.at[par])

    def gs_copy(unit, par):
        return pltpu.make_async_copy(gst.at[par], gs.at[unit], gs_sem.at[par])

    def stage(unit):
        layer = jnp.where(unit < per_layer, 1, 0)
        at = lax.rem(unit, per_layer) * PIECE
        rows = pl.ds(pl.multiple_of(me * (dm // n), dm // n), dm // n)
        copies = []
        for k, (w, m, v) in enumerate(((wg_hbm, mg_hbm, vg_hbm), (wu_hbm, mu_hbm, vu_hbm))):
            for d in range(n):
                cols = pl.ds(pl.multiple_of(d * share + at, PIECE), PIECE)
                to = pl.ds(d * PIECE, PIECE)
                copies += [(w.at[layer, rows, cols], w_st.at[k, :, to]), (m.at[layer, :, cols], m_st.at[k, :, to]), (v.at[layer, :, cols], v_st.at[k, :, to])]
        own = pl.ds(pl.multiple_of(at, PIECE), PIECE)
        copies += [
            (wd_hbm.at[layer, pl.ds(pl.multiple_of(me * share + at, PIECE), PIECE), :], w_st.at[2]),
            (md_hbm.at[layer, own, :], m_st.at[2]),
            (vd_hbm.at[layer, own, :], v_st.at[2]),
        ]
        return [pltpu.make_async_copy(src, dst, st_sem.at[i]) for i, (src, dst) in enumerate(copies)]

    def exchange():
        unit, older, oldest = u - 1, u - 2, u - 3
        par, opar = lax.rem(unit + 2, 2), lax.rem(older + 2, 2)
        summing = (unit >= 0) & (unit < units)
        sharing = (older >= 0) & (older < units)

        @pl.when((t == 0) & summing)
        def _():
            for copy in far(par) + plain(par):
                copy.start()

        @pl.when((t == 2) & (oldest >= 0))
        def _():
            for copy in out_far(oldest, par):
                copy.wait()

        @pl.when((t == 2) & summing)
        def _():
            for copy in far(par):
                copy.wait()
            for to, part, got in ((right, low, far_a), (left, high, far_b)):
                total = grads[par, to, :, part, :].astype(F32) + got[par].astype(F32)
                grads[par, to, :, part, :] = total.astype(BF16)
            for copy in joined(par):
                copy.start()
            for copy in stage(unit):
                copy.start()

        @pl.when((t == 2) & sharing)
        def _():
            for copy in out_first(older, opar):
                copy.wait()
            for copy in out_far(older, opar):
                copy.start()

        @pl.when((t == 3) & summing)
        def _():
            for copy in plain(par) + joined(par):
                copy.wait()
            for copy in stage(unit):
                copy.wait()

            @pl.when(unit >= 2)
            def _():
                gs_copy(unit - 2, par).wait()

            for k in range(3):
                total = grads[par, me, k].astype(F32) + near_a[par, k].astype(F32) + near_b[par, k].astype(F32)
                total = total.astype(BF16)
                gst[par, k] = total
                new_s[par, k] = step_of_adamw(w_st[k], m_st[k], v_st[k], total.astype(F32))
            for copy in out_first(unit, par) + out_second(unit, par):
                copy.start()
            own_copy(unit, par).start()
            gs_copy(unit, par).start()

        @pl.when((t == 3) & sharing)
        def _():
            for copy in out_second(older, opar):
                copy.wait()
            own_copy(older, opar).wait()

        @pl.when((t == 3) & (u == units + 1))
        def _():
            for copy in out_far(units - 1, 1):
                copy.wait()
            gs_copy(units - 2, 0).wait()
            gs_copy(units - 1, 1).wait()

    def init(k):
        rows = pl.ds(pl.multiple_of(k * TB, TB), TB)
        return (
            pltpu.make_async_copy(dy_hbm.at[0, rows, :], d_s.at[rows, :], init_sem.at[0, k]),
            pltpu.make_async_copy(dyt_hbm.at[:, rows], dt_s.at[:, rows], init_sem.at[1, k]),
        )

    @pl.when((u == 0) & (t == 0))
    def _():
        for k in range(d_s.shape[0] // TB):
            for copy in init(k):
                copy.start()
        barrier = pltpu.get_barrier_semaphore()
        for to in (left, right):
            pl.semaphore_signal(barrier, inc=1, device_id={"dp": to}, device_id_type=MESH)
        pl.semaphore_wait(barrier, 2)

    @pl.when(u == 0)
    def _():
        for copy in init(t):
            copy.wait()

    @pl.when((u < units) & (t == 0))
    def _():
        accg[...] = jnp.zeros_like(accg)
        accu[...] = jnp.zeros_like(accu)
        accd[...] = jnp.zeros_like(accd)
        for k in range(n):
            to = pl.ds(k * PIECE, PIECE)
            wg_s[:, to] = wg_refs[k][0]
            wu_s[:, to] = wu_refs[k][0]
            wd_s[to, :] = wd_refs[k][0]

    here = pl.ds(pl.multiple_of(t * TB, TB), TB)

    @pl.when(u == 0)
    def _():
        da_s[here, :] = jnp.zeros((TB, dm), F32)

    def compute(i, with_da):
        rows = pl.ds(i * SUB, SUB)
        sub = pl.ds(pl.multiple_of(t * TB + i * SUB, SUB), SUB)
        wg, wu, wd = wg_s[...], wu_s[...], wd_s[...]
        a, d = a_ref[0, rows, :], d_s[sub, :]
        gate = dot(a, wg)
        up = dot(a, wu)
        dp = dot_nt(d, wd).astype(BF16).astype(F32)
        s = lax.logistic(gate)
        silu = gate * s
        p = (silu * up).astype(BF16)
        dup = (dp * silu).astype(BF16)
        dgate = (dp * up * (s + silu * (1.0 - s))).astype(BF16)
        at = at_ref[0, :, rows]
        accg[...] += dot(at, dgate)
        accu[...] += dot(at, dup)
        accd[...] += dot(dt_s[:, sub], p)
        if with_da:
            da_s[sub, :] += dot_nt(dgate, wg) + dot_nt(dup, wu)

    exchange()

    @pl.when(u < per_layer)
    def _():
        for i in range(TB // SUB):
            compute(i, True)

    @pl.when((u >= per_layer) & (u < units))
    def _():
        for i in range(TB // SUB):
            compute(i, False)

    @pl.when((u < units) & (t == nt - 1))
    def _():
        par = lax.rem(u, 2)
        for k in range(n):
            part = pl.ds(k * PIECE, PIECE)
            grads[par, k, 0] = accg[part, :].astype(BF16)
            grads[par, k, 1] = accu[part, :].astype(BF16)
            grads[par, k, 2] = accd[:, part].astype(BF16).T

    @pl.when(u == per_layer - 1)
    def _():
        da = da_s[here, :].astype(BF16).astype(F32)
        wide = h_ref[...].astype(F32)
        scale = lax.rsqrt(jnp.mean(wide * wide, -1, keepdims=True) + 1e-6)
        along = jnp.mean(da * wide, -1, keepdims=True)
        dn = (da * scale - wide * (along * (scale * scale * scale))).astype(BF16)
        dh = d_s[here, :] + dn
        d_s[here, :] = dh
        dt_s[:, here] = dh.T


def backward(n, a, at, h, dy, dyt, wg, wu, wd, moments):
    _, tokens, dm = a.shape
    layers, _, ff = wg.shape
    nt = tokens // TB
    f = n * PIECE
    per_layer = ff // f
    units = layers * per_layer
    now = lambda u: jnp.minimum(u, units - 1)
    layer = lambda u: jnp.where(u < per_layer, 1, 0)
    piece = lambda k: lambda u, t: (layer(u), 0, k * per_layer + lax.rem(now(u), per_layer))
    piece_t = lambda k: lambda u, t: (layer(u), k * per_layer + lax.rem(now(u), per_layer), 0)
    step = lambda u, t: jnp.where(u < units, t, nt - 1)
    hbm = pl.BlockSpec(memory_space=pl.ANY)
    in_specs = [
        pl.BlockSpec((1, TB, dm), lambda u, t: (layer(u), step(u, t), 0)),
        pl.BlockSpec((1, dm, TB), lambda u, t: (layer(u), 0, step(u, t))),
        pl.BlockSpec((TB, dm), lambda u, t: (jnp.where(u == per_layer - 1, t, jnp.where(u < per_layer, 0, nt - 1)), 0)),
        *[pl.BlockSpec((1, dm, PIECE), piece(k)) for k in range(n)] * 1,
        *[pl.BlockSpec((1, dm, PIECE), piece(k)) for k in range(n)],
        *[pl.BlockSpec((1, PIECE, dm), piece_t(k)) for k in range(n)],
        *[hbm] * 11,
    ]
    chunk = (3, PIECE, dm)
    part = (3, PIECE // 2, dm)
    dma = pltpu.SemaphoreType.DMA
    return pl.pallas_call(
        functools.partial(bwd_kernel, n, per_layer),
        grid=(units + 2, nt),
        in_specs=in_specs,
        out_specs=[hbm, hbm],
        out_shape=[jax.ShapeDtypeStruct((units, n, *chunk), BF16), jax.ShapeDtypeStruct((units, *chunk), BF16)],
        scratch_shapes=[
            pltpu.VMEM((tokens, dm), BF16),
            pltpu.VMEM((dm, tokens), BF16),
            pltpu.VMEM((tokens, dm), F32),
            pltpu.VMEM((dm, f), BF16),
            pltpu.VMEM((dm, f), BF16),
            pltpu.VMEM((f, dm), BF16),
            pltpu.VMEM((dm, f), F32),
            pltpu.VMEM((dm, f), F32),
            pltpu.VMEM((dm, f), F32),
            pltpu.VMEM((2, n, *chunk), BF16),
            pltpu.VMEM((2, *part), BF16),
            pltpu.VMEM((2, *part), BF16),
            pltpu.VMEM((2, *chunk), BF16),
            pltpu.VMEM((2, *chunk), BF16),
            pltpu.VMEM((2, *chunk), BF16),
            pltpu.VMEM((2, *chunk), BF16),
            pltpu.VMEM(chunk, BF16),
            pltpu.VMEM(chunk, F32),
            pltpu.VMEM(chunk, F32),
            dma((2, nt)),
            dma((12, 2)),
            dma((12, 2)),
            dma((6 * n + 3,)),
            dma((2,)),
            dma((2,)),
        ],
        compiler_params=pltpu.CompilerParams(
            vmem_limit_bytes=VMEM, dimension_semantics=("arbitrary", "arbitrary"), collective_id=0, has_side_effects=True
        ),
        cost_estimate=pl.CostEstimate(flops=14 * layers * tokens * dm * ff, bytes_accessed=12 * tokens * ff, transcendentals=layers * tokens * ff),
        name="backward",
    )(a, at, h, *[wg] * n, *[wu] * n, *[wd] * n, dy, dyt, wg, wu, wd, *moments)


def finish_kernel(n, per_layer, wag, gs, *refs):
    olds, outs = refs[:6], refs[6:]
    q = pl.program_id(1)
    share = per_layer * PIECE
    rows = outs[3].shape[1]
    lanes = outs[5].shape[2]
    mine = pl.ds(pl.multiple_of(q * rows, rows), rows)
    some = pl.ds(pl.multiple_of(q * lanes, lanes), lanes)

    def moments(k, where, g):
        g = g.astype(F32)
        outs[3 + k][where] = 0.9 * olds[k][where] + 0.1 * g
        outs[6 + k][where] = 0.95 * olds[3 + k][where] + 0.05 * g * g

    for j in range(per_layer):
        down = pl.ds(j * PIECE, PIECE)
        outs[2][0, down, :] = wag[j, 0, 2]
        moments(2, (0, down, slice(None)), gs[j, 2, :, some])
        for d in range(n):
            cols = pl.ds(d * share + j * PIECE, PIECE)
            for k in range(2):
                outs[k][0, :, cols] = wag[j, 0, k, :, d * PIECE : (d + 1) * PIECE]
                moments(k, (0, slice(None), cols), gs[j, k, mine, d * PIECE : (d + 1) * PIECE])


def finish(n, wag, gs, olds):
    units, _, _, _, dm = wag.shape
    layers, rows, ff = olds[0].shape
    per_layer = units // layers
    share = per_layer * PIECE
    small = [pl.BlockSpec((1, rows // n, ff), lambda l, q: (l, q, 0))] * 2 + [pl.BlockSpec((1, share, dm // n), lambda l, q: (l, 0, q))]
    whole = [pl.BlockSpec((1, rows, ff), lambda l, q: (l, q, 0))] * 2 + [pl.BlockSpec((1, share, dm), lambda l, q: (l, q, 0))]
    return pl.pallas_call(
        functools.partial(finish_kernel, n, per_layer),
        grid=(layers, n),
        in_specs=[
            pl.BlockSpec((per_layer, 1, 3, PIECE, dm), lambda l, q: (layers - 1 - l, q, 0, 0, 0)),
            pl.BlockSpec((per_layer, 3, PIECE, dm), lambda l, q: (layers - 1 - l, 0, 0, 0)),
            *small,
            *small,
        ],
        out_specs=[*whole, *small, *small],
        out_shape=[jax.ShapeDtypeStruct((layers, dm, ff), BF16)] * 2
        + [jax.ShapeDtypeStruct((layers, ff, dm), BF16)]
        + [jax.ShapeDtypeStruct(one.shape, F32) for one in olds],
        compiler_params=pltpu.CompilerParams(vmem_limit_bytes=VMEM, dimension_semantics=("arbitrary", "arbitrary")),
        name="finish",
    )(wag, gs, *olds)


def solution(mesh):
    n = mesh.shape["dp"]

    def step(x, dy, wg, wu, wd, *olds):
        h, a, at, dyt = forward(x, dy, wg, wu, wd)
        wag, gs = backward(n, a, at, h, dy, dyt, wg, wu, wd, olds)
        return tuple(finish(n, wag, gs, olds))

    whole = P(None, None, None)
    rows = P(None, "dp", None)
    seq = P(("rep", "dp"), None, None)
    return jax.shard_map(
        step,
        mesh=mesh,
        in_specs=(seq, seq, whole, whole, whole, *[rows] * 6),
        out_specs=(*[P("rep", None, None)] * 3, *[P("rep", "dp", None)] * 6),
        check_vma=False,
    )
```
